8 devices in a mesh: col: 2 (over z, y), row: 4 (over x, core).
Axes of the slice: x: 2, y: 2, z: 1, core: 2. Of those that a mesh axis runs over, the one named last changes fastest.
Arguments:
- psi_start: float32 [2048, 2, 2, 2048], P('row', None, None, 'col')
- left_env: float32 [2048, 8, 2048], P('row')
- right_env: float32 [2048, 8, 2048], P('col')
- mpo_pair: float32 [8, 8, 2, 2, 2, 2], replicated
Outputs:
- output 1: float32 [4], replicated
- output 2: float32 [4], replicated
- output 3: float32 [2048, 2, 2, 2048], P('row', None, None, 'col')
All inputs are finite; a program needn't handle non-finite values.
Results may differ from the reference program's by a relative error of at most 0.001.
Values sent between devices are 32-bit elements.
A program may use at most 1 GiB of HBM per device.

```python
import jax
import jax.numpy as jnp
from jax import lax

BOND_DIM = 2048
PHYS_DIM = 2
MPO_DIM = 8
LANCZOS_STEPS = 4

FULL_PREC = lax.Precision.HIGHEST


def symmetric_env(key_rand, key_diag):
    rand_part = jax.random.normal(key_rand, (BOND_DIM, MPO_DIM, BOND_DIM), jnp.float32)
    sym_part = (rand_part + jnp.transpose(rand_part, (2, 1, 0))) * (2.0 * BOND_DIM) ** -0.5
    diag_part = jax.random.normal(key_diag, (MPO_DIM,), jnp.float32)
    identity = jnp.eye(BOND_DIM, dtype=jnp.float32)
    return sym_part + identity[:, None, :] * diag_part[None, :, None]


def symmetric_mpo(key_rand, key_diag):
    loc_dim = PHYS_DIM * PHYS_DIM
    rand_part = jax.random.normal(key_rand, (MPO_DIM, MPO_DIM, loc_dim, loc_dim), jnp.float32)
    diag_part = jax.random.normal(key_diag, (MPO_DIM, MPO_DIM), jnp.float32)
    identity = jnp.eye(loc_dim, dtype=jnp.float32)
    sym_part = (rand_part + jnp.swapaxes(rand_part, 2, 3)) * 0.5 ** 0.5
    full_mpo = (sym_part + diag_part[:, :, None, None] * identity) / (MPO_DIM * PHYS_DIM)
    return full_mpo.reshape(MPO_DIM, MPO_DIM, PHYS_DIM, PHYS_DIM, PHYS_DIM, PHYS_DIM)


def setup_inputs(seed: int = 0) -> dict:
    key_list = jax.random.split(jax.random.key(seed), 7)
    psi_start = jax.random.normal(key_list[0], (BOND_DIM, PHYS_DIM, PHYS_DIM, BOND_DIM), jnp.float32)
    return {'psi_start': psi_start, 'left_env': symmetric_env(key_list[1], key_list[2]), 'right_env': symmetric_env(key_list[3], key_list[4]), 'mpo_pair': symmetric_mpo(key_list[5], key_list[6])}


def apply_ham(left_env, right_env, mpo_pair, vec_in):
    block_count = 8
    block_len = BOND_DIM // block_count
    left_blocks = jnp.transpose(left_env.reshape(BOND_DIM, MPO_DIM, block_count, block_len), (2, 0, 1, 3))

    def one_block(left_blk):
        stage_one = jnp.einsum('alc,asub->lcsub', left_blk.astype(jnp.float32), vec_in.astype(jnp.float32), precision=FULL_PREC)
        stage_two = jnp.einsum('lrsutq,lcsub->rctqb', mpo_pair.astype(jnp.float32), stage_one, precision=FULL_PREC)
        return jnp.einsum('rctqb,bre->ctqe', stage_two, right_env.astype(jnp.float32), precision=FULL_PREC)

    out_blocks = lax.map(one_block, left_blocks)
    return out_blocks.reshape(BOND_DIM, PHYS_DIM, PHYS_DIM, BOND_DIM)


def reference(psi_start, left_env, right_env, mpo_pair):
    num_elems = float(PHYS_DIM * PHYS_DIM * BOND_DIM * BOND_DIM)

    def mean_dot(left_vec, right_vec):
        return jnp.sum(left_vec * right_vec) / num_elems

    start_vec = psi_start * lax.rsqrt(mean_dot(psi_start, psi_start))

    def lanczos_step(carry, unused):
        prev_vec, cur_vec, prev_beta = carry
        h_vec = apply_ham(left_env, right_env, mpo_pair, cur_vec)
        alpha_j = mean_dot(cur_vec, h_vec)
        residual = h_vec - alpha_j * cur_vec - prev_beta * prev_vec
        beta_j = jnp.sqrt(mean_dot(residual, residual))
        return (cur_vec, residual / beta_j, beta_j), (alpha_j, beta_j)

    init_carry = (jnp.zeros_like(start_vec), start_vec, jnp.zeros((), jnp.float32))
    final_carry, history = lax.scan(lanczos_step, init_carry, None, length=LANCZOS_STEPS)
    return history[0], history[1], final_carry[1]
```

```python
import jax
import jax.numpy as jnp
from jax import lax
from jax.experimental import pallas as pl
from jax.experimental.pallas import tpu as pltpu
from jax.sharding import PartitionSpec as P

LANCZOS_STEPS = 4
FULL_PREC = lax.Precision.HIGHEST
MESH_ID = pl.DeviceIdType.MESH
F32 = jnp.float32
VMEM_LIMIT = 60 << 20

COL, ROW = 2, 4
NDEV = COL * ROW
W_DIM = 8
S_DIM = 4
A_LOC = 512
A_ALL = A_LOC * ROW
B_LOC = 1024
B_ALL = B_LOC * COL
HALF = B_LOC // 2
V_ROWS = S_DIM * A_LOC
NUM_ELEMS = float(A_ALL * S_DIM * B_ALL)

C_TILE = 64
B_TILE = 256
GROUP = 8


def sds(*shape):
    return jax.ShapeDtypeStruct(shape, F32)


def dot(lhs, rhs):
    return jnp.dot(lhs, rhs, precision=FULL_PREC, preferred_element_type=F32)


def stage_one_body(left_ref, vec_ref, mpo_ref, *rest):
    out_ref, part_ref = rest[-2:]
    per_dot = 2
    width = per_dot * B_TILE
    for pair in range(S_DIM // per_dot):
        cols = []
        for s in range(pair * per_dot, (pair + 1) * per_dot):
            cols.append(jnp.concatenate([vec_ref[i, s] for i in range(ROW)], axis=0))
        part_ref[:, pair * width:(pair + 1) * width] = dot(left_ref[...], jnp.concatenate(cols, axis=1))
    n_grp = C_TILE // GROUP
    rows = GROUP * W_DIM
    stacked = []
    for g in range(n_grp):
        pieces = [part_ref[g * rows:(g + 1) * rows, s * B_TILE:(s + 1) * B_TILE] for s in range(S_DIM)]
        stacked.append(jnp.concatenate(pieces, axis=0))
    res = dot(mpo_ref[...], jnp.concatenate(stacked, axis=1))
    for g in range(n_grp):
        for r in range(W_DIM):
            for t in range(S_DIM):
                r0 = (r * S_DIM + t) * GROUP
                out_ref[r, t, g * GROUP:(g + 1) * GROUP, :] = res[r0:r0 + GROUP, g * B_TILE:(g + 1) * B_TILE]


def stage_one(left_rows, vec, mpo_big, half, prev):
    n_b = HALF // B_TILE
    in_specs = [
        pl.BlockSpec((C_TILE * W_DIM, A_ALL), lambda b, c: (c, 0)),
        pl.BlockSpec((ROW, S_DIM, A_LOC, B_TILE), lambda b, c: (0, 0, 0, b)),
        pl.BlockSpec((256, 256), lambda b, c: (0, 0)),
    ]
    args = [left_rows, vec, mpo_big]
    alias = {}
    if prev is not None:
        in_specs.append(pl.BlockSpec(memory_space=pl.ANY))
        args.append(prev)
        alias = {3: 0}
    base = half * n_b
    return pl.pallas_call(
        stage_one_body,
        grid=(n_b, A_LOC // C_TILE),
        in_specs=in_specs,
        out_specs=pl.BlockSpec((W_DIM, S_DIM, C_TILE, B_TILE), lambda b, c: (0, 0, c, b + base)),
        out_shape=sds(W_DIM, S_DIM, A_LOC, B_LOC),
        scratch_shapes=[pltpu.VMEM((C_TILE * W_DIM, S_DIM * B_TILE), F32)],
        input_output_aliases=alias,
        compiler_params=pltpu.CompilerParams(vmem_limit_bytes=VMEM_LIMIT),
        cost_estimate=pl.CostEstimate(flops=6 * 2 * A_LOC * W_DIM * A_ALL * S_DIM * HALF, bytes_accessed=150 << 20, transcendentals=0),
        name='stage_one',
    )(*args)


S3_M = 1024
S3_R = 2


def stage_three_body(sel_ref, t2_ref, right_ref, *rest):
    out_ref = rest[-1]
    acc = dot(t2_ref[0], right_ref[0])
    for i in range(1, S3_R):
        acc = acc + dot(t2_ref[i], right_ref[i])
    first = pl.program_id(1) == 0
    out_ref[...] = jnp.where(first, 0.0, out_ref[...]) + acc


def stage_three(t2, right_t, block, after):
    in_specs = [
        pl.BlockSpec((S3_R, S3_M, B_LOC), lambda m, k, sel: (k, m, 0)),
        pl.BlockSpec((S3_R, B_LOC, HALF), lambda m, k, sel: (k, 0, sel[0])),
    ]
    args = [block, t2, right_t]
    if after is not None:
        in_specs.append(pl.BlockSpec(memory_space=pl.ANY))
        args.append(after)
    return pl.pallas_call(
        stage_three_body,
        grid_spec=pltpu.PrefetchScalarGridSpec(
            num_scalar_prefetch=1,
            grid=(V_ROWS // S3_M, W_DIM // S3_R),
            in_specs=in_specs,
            out_specs=pl.BlockSpec((S3_M, HALF), lambda m, k, sel: (m, 0)),
        ),
        out_shape=sds(V_ROWS, HALF),
        compiler_params=pltpu.CompilerParams(vmem_limit_bytes=VMEM_LIMIT),
        cost_estimate=pl.CostEstimate(flops=6 * 2 * V_ROWS * W_DIM * B_LOC * HALF, bytes_accessed=90 << 20, transcendentals=0),
        name='stage_three',
    )(*args)


def relayout_body(in_ref, out_ref):
    for r in range(W_DIM):
        out_ref[r] = in_ref[:, r, :]


def relayout(right_blk):
    b_t, e_t = 128, 1024
    return pl.pallas_call(
        relayout_body,
        grid=(B_LOC // b_t, B_ALL // e_t),
        in_specs=[pl.BlockSpec((b_t, W_DIM, e_t), lambda b, e: (b, 0, e))],
        out_specs=pl.BlockSpec((W_DIM, b_t, e_t), lambda b, e: (0, b, e)),
        out_shape=sds(W_DIM, B_LOC, B_ALL),
        compiler_params=pltpu.CompilerParams(vmem_limit_bytes=VMEM_LIMIT),
        cost_estimate=pl.CostEstimate(flops=1 << 34, bytes_accessed=128 << 20, transcendentals=0),
        name='relayout',
    )(right_blk)


CHUNKS = 8
CH_ROWS = V_ROWS // CHUNKS
STEP_ROWS = 32


def enter_all():
    barrier = pltpu.get_barrier_semaphore()
    me = lax.axis_index('col') * ROW + lax.axis_index('row')
    for d in range(1, NDEV):
        peer = lax.rem(me + d, NDEV)
        pl.semaphore_signal(barrier, inc=1, device_id=(peer // ROW, lax.rem(peer, ROW)), device_id_type=MESH_ID)
    return me, barrier


def all_mean(me, part, slots, send_sem, recv_sem):
    slots[me] = part
    copies = []
    for d in range(1, NDEV):
        peer = lax.rem(me + d, NDEV)
        copy = pltpu.make_async_remote_copy(
            src_ref=slots.at[me], dst_ref=slots.at[me], send_sem=send_sem.at[d], recv_sem=recv_sem.at[me],
            device_id=(peer // ROW, lax.rem(peer, ROW)), device_id_type=MESH_ID)
        copy.start()
        copies.append(copy)
    for d in range(1, NDEV):
        src = lax.rem(me + d, NDEV)
        pltpu.make_async_remote_copy(
            src_ref=slots.at[src], dst_ref=slots.at[src], send_sem=send_sem.at[d], recv_sem=recv_sem.at[src],
            device_id=(src // ROW, lax.rem(src, ROW)), device_id_type=MESH_ID).wait_recv()
    for copy in copies:
        copy.wait_send()
    total = slots[0]
    for i in range(1, NDEV):
        total = total + slots[i]
    total = jnp.sum(jnp.sum(total, axis=0, keepdims=True), axis=1, keepdims=True)
    return jnp.broadcast_to(total, (8, 128)) * (1.0 / NUM_ELEMS)


def fold(x):
    rows = x[0:8]
    for i in range(1, x.shape[0] // 8):
        rows = rows + x[i * 8:(i + 1) * 8]
    out = rows[:, 0:128]
    for i in range(1, rows.shape[1] // 128):
        out = out + rows[:, i * 128:(i + 1) * 128]
    return out


def row_loop(start, rows, body, init):
    def step(i, carry):
        r0 = pl.multiple_of(start + i * STEP_ROWS, STEP_ROWS)
        return body(pl.ds(r0, STEP_ROWS), carry)
    return lax.fori_loop(0, rows // STEP_ROWS, step, init)


def as_scalar_tile(x):
    return jnp.broadcast_to(x[0:1, 0:1], (STEP_ROWS, HALF))


def start_norm_body(psi_ref, out_a, out_c, vec, in_sem, out_sem, slots, send_sem, recv_sem):
    me, barrier = enter_all()
    loads = []
    for k in range(CHUNKS):
        rows = pl.ds(k * CH_ROWS, CH_ROWS)
        load = pltpu.make_async_copy(psi_ref.at[rows, :], vec.at[rows, :], in_sem.at[k])
        load.start()
        loads.append(load)
    acc = jnp.zeros((8, 128), F32)
    for k in range(CHUNKS):
        loads[k].wait()

        def body(rows, carry):
            x = vec[rows, :]
            return carry + fold(x * x)
        acc = row_loop(k * CH_ROWS, CH_ROWS, body, acc)
    pl.semaphore_wait(barrier, NDEV - 1)
    inv = lax.rsqrt(all_mean(me, acc, slots, send_sem, recv_sem))
    scale = as_scalar_tile(inv)
    stores = []
    for k in range(CHUNKS):
        def body(rows, carry):
            vec[rows, 0:HALF] = vec[rows, 0:HALF] * scale
            vec[rows, HALF:B_LOC] = vec[rows, HALF:B_LOC] * scale
            return carry
        row_loop(k * CH_ROWS, CH_ROWS, body, 0)
        rows = pl.ds(k * CH_ROWS, CH_ROWS)
        for h, out in enumerate((out_a, out_c)):
            store = pltpu.make_async_copy(vec.at[rows, pl.ds(h * HALF, HALF)], out.at[rows, :], out_sem.at[h, k])
            store.start()
            stores.append(store)
    for store in stores:
        store.wait()


def start_norm(psi_rows):
    any_spec = pl.BlockSpec(memory_space=pl.ANY)
    return pl.pallas_call(
        start_norm_body,
        in_specs=[any_spec],
        out_specs=[any_spec, any_spec],
        out_shape=[sds(V_ROWS, HALF), sds(V_ROWS, HALF)],
        scratch_shapes=[
            pltpu.VMEM((V_ROWS, B_LOC), F32),
            pltpu.SemaphoreType.DMA((CHUNKS,)),
            pltpu.SemaphoreType.DMA((2, CHUNKS)),
            pltpu.VMEM((NDEV, 8, 128), F32),
            pltpu.SemaphoreType.DMA((NDEV,)),
            pltpu.SemaphoreType.DMA((NDEV,)),
        ],
        compiler_params=pltpu.CompilerParams(collective_id=0, has_side_effects=True, vmem_limit_bytes=VMEM_LIMIT),
        cost_estimate=pl.CostEstimate(flops=1 << 32, bytes_accessed=16 << 20, transcendentals=0),
        name='start_norm',
    )(psi_rows)


def lanczos_body(n_prev, h_a, own_c, recv_c, v_a, v_c, *rest):
    prevs = rest[:2] if n_prev else ()
    rest = rest[2:] if n_prev else rest
    beta_prev, rest = (rest[0], rest[1:]) if n_prev else (None, rest)
    out_a, out_c, alpha_ref, beta_ref = rest[:4]
    if n_prev:
        hv, rv, vv, pv, in_sem, out_sem, slots, slots2, send_sem, recv_sem, send_sem2, recv_sem2 = rest[4:]
    else:
        hv, rv, vv, in_sem, out_sem, slots, slots2, send_sem, recv_sem, send_sem2, recv_sem2 = rest[4:]
        pv = None
    me, barrier = enter_all()
    lo, hi = pl.ds(0, HALF), pl.ds(HALF, HALF)
    loads = []
    for k in range(CHUNKS):
        rows = pl.ds(k * CH_ROWS, CH_ROWS)
        group = []
        moves = [(h_a, hv.at[rows, lo]), (own_c, hv.at[rows, hi]), (recv_c, rv.at[rows, :]), (v_a, vv.at[rows, lo]), (v_c, vv.at[rows, hi])]
        for i, (src, dst) in enumerate(moves):
            load = pltpu.make_async_copy(src.at[rows, :], dst, in_sem.at[k, i])
            load.start()
            group.append(load)
        loads.append(group)
    late = []
    if n_prev:
        for k in range(CHUNKS):
            rows = pl.ds(k * CH_ROWS, CH_ROWS)
            for i, (src, cols) in enumerate(((prevs[0], lo), (prevs[1], hi))):
                load = pltpu.make_async_copy(src.at[rows, :], pv.at[rows, cols], in_sem.at[k, 5 + i])
                load.start()
                late.append(load)
    acc = jnp.zeros((8, 128), F32)
    for k in range(CHUNKS):
        for load in loads[k]:
            load.wait()

        def body(rows, carry):
            h_c = hv[rows, HALF:B_LOC] + rv[rows, :]
            hv[rows, HALF:B_LOC] = h_c
            return carry + fold(hv[rows, 0:HALF] * vv[rows, 0:HALF] + h_c * vv[rows, HALF:B_LOC])
        acc = row_loop(k * CH_ROWS, CH_ROWS, body, acc)
    pl.semaphore_wait(barrier, NDEV - 1)
    alpha = all_mean(me, acc, slots, send_sem, recv_sem)
    alpha_ref[...] = alpha
    for load in late:
        load.wait()
    alpha_t = as_scalar_tile(alpha)
    beta_t = as_scalar_tile(beta_prev[...]) if n_prev else None

    def residual(rows, carry):
        for c0 in (0, HALF):
            w = hv[rows, c0:c0 + HALF] - alpha_t * vv[rows, c0:c0 + HALF]
            if n_prev:
                w = w - beta_t * pv[rows, c0:c0 + HALF]
            hv[rows, c0:c0 + HALF] = w
            carry = carry + fold(w * w)
        return carry
    acc = row_loop(0, V_ROWS, residual, jnp.zeros((8, 128), F32))
    beta = jnp.sqrt(all_mean(me, acc, slots2, send_sem2, recv_sem2))
    beta_ref[...] = beta
    inv_t = as_scalar_tile(1.0 / beta)
    stores = []
    for k in range(CHUNKS):
        def scale_rows(rows, carry):
            for c0 in (0, HALF):
                hv[rows, c0:c0 + HALF] = hv[rows, c0:c0 + HALF] * inv_t
            return carry
        row_loop(k * CH_ROWS, CH_ROWS, scale_rows, 0)
        rows = pl.ds(k * CH_ROWS, CH_ROWS)
        for h, out in enumerate((out_a, out_c)):
            store = pltpu.make_async_copy(hv.at[rows, pl.ds(h * HALF, HALF)], out.at[rows, :], out_sem.at[h, k])
            store.start()
            stores.append(store)
    for store in stores:
        store.wait()


def lanczos_update(step_idx, h_a, own_c, recv_c, v_a, v_c, prev):
    n_prev = 0 if prev is None else 1
    any_spec = pl.BlockSpec(memory_space=pl.ANY)
    tile_spec = pl.BlockSpec(memory_space=pltpu.VMEM)
    args = [h_a, own_c, recv_c, v_a, v_c]
    in_specs = [any_spec] * 5
    if n_prev:
        args += list(prev)
        in_specs += [any_spec, any_spec, tile_spec]
    big = pltpu.VMEM((V_ROWS, B_LOC), F32)
    return pl.pallas_call(
        lambda *refs: lanczos_body(n_prev, *refs),
        in_specs=in_specs,
        out_specs=[any_spec, any_spec, tile_spec, tile_spec],
        out_shape=[sds(V_ROWS, HALF), sds(V_ROWS, HALF), sds(8, 128), sds(8, 128)],
        scratch_shapes=[big, pltpu.VMEM((V_ROWS, HALF), F32), big] + [big] * n_prev + [
            pltpu.SemaphoreType.DMA((CHUNKS, 7)),
            pltpu.SemaphoreType.DMA((2, CHUNKS)),
            pltpu.VMEM((NDEV, 8, 128), F32),
            pltpu.VMEM((NDEV, 8, 128), F32),
            pltpu.SemaphoreType.DMA((NDEV,)),
            pltpu.SemaphoreType.DMA((NDEV,)),
            pltpu.SemaphoreType.DMA((NDEV,)),
            pltpu.SemaphoreType.DMA((NDEV,)),
        ],
        compiler_params=pltpu.CompilerParams(collective_id=1 + step_idx, has_side_effects=True, vmem_limit_bytes=VMEM_LIMIT),
        cost_estimate=pl.CostEstimate(flops=1 << 33, bytes_accessed=40 << 20, transcendentals=0),
        name='lanczos_update',
    )(*args)


def gather_rows(x):
    return lax.all_gather(x.reshape(S_DIM, A_LOC, HALF), 'row', axis=0, tiled=False)


def solution(mesh):
    swap = [(0, 1), (1, 0)]

    def local_run(psi_blk, left_blk, right_blk, mpo_pair):
        col = lax.axis_index('col').astype(jnp.int32)
        left_rows = left_blk.reshape(A_LOC * W_DIM, A_ALL)
        mpo4 = mpo_pair.reshape(W_DIM, W_DIM, S_DIM, S_DIM).transpose(1, 3, 2, 0)
        same_c = jnp.eye(GROUP, dtype=jnp.bool_)[None, None, :, None, :, None]
        mpo_big = jnp.where(same_c, mpo4[:, :, None, :, None, :], 0.0).reshape(256, 256)

        psi_rows = psi_blk.reshape(A_LOC, S_DIM, B_LOC).transpose(1, 0, 2).reshape(V_ROWS, B_LOC)
        v_a, v_c = start_norm(psi_rows)
        g_a = gather_rows(v_a)
        g_c = gather_rows(v_c)
        right_t = relayout(right_blk)

        prev = None
        g_prev = None
        alpha_list, beta_list = [], []
        for step_idx in range(LANCZOS_STEPS):
            last = step_idx == LANCZOS_STEPS - 1
            t2 = stage_one(left_rows, g_a, mpo_big, 0, None)
            t2 = stage_one(left_rows, g_c, mpo_big, 1, t2)
            t2 = t2.reshape(W_DIM, V_ROWS, B_LOC)
            mine = [(2 * col + i).reshape(1) for i in range(2)]
            theirs = [(2 * (1 - col) + i).reshape(1) for i in range(2)]
            oth_a = stage_three(t2, right_t, theirs[0], None)
            recv_a = lax.ppermute(oth_a, 'col', swap)
            oth_c = stage_three(t2, right_t, theirs[1], oth_a)
            recv_c = lax.ppermute(oth_c, 'col', swap)
            own_a = stage_three(t2, right_t, mine[0], oth_c)
            h_a = own_a + recv_a
            if not last:
                h_all = gather_rows(h_a)
            own_c = stage_three(t2, right_t, mine[1], h_a)
            n_a, n_c, alpha, beta = lanczos_update(step_idx, h_a, own_c, recv_c, v_a, v_c, prev)
            alpha_list.append(alpha[0, 0])
            beta_list.append(beta[0, 0])
            if not last:
                w_all = h_all - alpha[0, 0] * g_a
                if g_prev is not None:
                    w_all = w_all - beta_list[-2] * g_prev
                g_prev = g_a
                g_a = w_all * (1.0 / beta[0, 0])
                g_c = gather_rows(n_c)
            prev = (v_a, v_c, beta)
            v_a, v_c = n_a, n_c
        out = jnp.concatenate([v_a.reshape(S_DIM, A_LOC, HALF), v_c.reshape(S_DIM, A_LOC, HALF)], axis=2)
        out = out.transpose(1, 0, 2).reshape(A_LOC, 2, 2, B_LOC)
        return jnp.stack(alpha_list), jnp.stack(beta_list), out

    return jax.shard_map(local_run, mesh=mesh, in_specs=(P('row', None, None, 'col'), P('row', None, None), P('col', None, None), P()), out_specs=(P(), P(), P('row', None, None, 'col')), check_vma=False)
```

```python
import jax
import jax.numpy as jnp
from jax import lax
from jax.experimental import pallas as pl
from jax.experimental.pallas import tpu as pltpu
from jax.sharding import PartitionSpec as P


LANCZOS_STEPS = 4
FULL_PREC = lax.Precision.HIGHEST
MESH_ID = pl.DeviceIdType.MESH
F32 = jnp.float32
VMEM_LIMIT = 60 << 20

COL, ROW = 2, 4
NDEV = COL * ROW
W_DIM = 8
S_DIM = 4
A_LOC = 512
A_ALL = A_LOC * ROW
B_LOC = 1024
B_ALL = B_LOC * COL
HALF = B_LOC // 2
V_ROWS = S_DIM * A_LOC
NUM_ELEMS = float(A_ALL * S_DIM * B_ALL)

C_TILE = 64
B_TILE = 256
GROUP = 8
STAGE_THREE_FLOPS = 6 * 2 * V_ROWS * W_DIM * B_LOC * HALF


def sds(*shape):
    return jax.ShapeDtypeStruct(shape, F32)


def dot(lhs, rhs):
    return jnp.dot(lhs, rhs, precision=FULL_PREC, preferred_element_type=F32)


def first_two_stages(left_ref, vec_of, mpo_ref, out_ref, part_ref):
    per_dot = 2
    width = per_dot * B_TILE
    for pair in range(S_DIM // per_dot):
        cols = []
        for s in range(pair * per_dot, (pair + 1) * per_dot):
            cols.append(jnp.concatenate([vec_of(i, s) for i in range(ROW)], axis=0))
        part_ref[:, pair * width:(pair + 1) * width] = dot(left_ref[...], jnp.concatenate(cols, axis=1))
    n_grp = left_ref.shape[0] // (W_DIM * GROUP)
    rows = GROUP * W_DIM
    stacked = []
    for g in range(n_grp):
        pieces = [part_ref[g * rows:(g + 1) * rows, s * B_TILE:(s + 1) * B_TILE] for s in range(S_DIM)]
        stacked.append(jnp.concatenate(pieces, axis=0))
    res = dot(mpo_ref[...], jnp.concatenate(stacked, axis=1))
    for g in range(n_grp):
        for r in range(W_DIM):
            for t in range(S_DIM):
                r0 = (r * S_DIM + t) * GROUP
                out_ref[r, t, g * GROUP:(g + 1) * GROUP, :] = res[r0:r0 + GROUP, g * B_TILE:(g + 1) * B_TILE]


def stage_one_body(left_ref, vec_ref, mpo_ref, *rest):
    out_ref, part_ref = rest[-2:]
    first_two_stages(left_ref, lambda i, s: vec_ref[i, s], mpo_ref, out_ref, part_ref)


MPO_SPEC = pl.BlockSpec((256, 256), lambda b, c: (0, 0))
ANY_SPEC = pl.BlockSpec(memory_space=pl.ANY)
TILE_SPEC = pl.BlockSpec(memory_space=pltpu.VMEM)


def left_spec(c_tile):
    return pl.BlockSpec((c_tile * W_DIM, A_ALL), lambda b, c: (c, 0))


def stage_one_cost(width):
    return pl.CostEstimate(flops=6 * 2 * A_LOC * W_DIM * A_ALL * S_DIM * width, bytes_accessed=150 << 20, transcendentals=0)


def stage_one(left_rows, vec, mpo_big, base, prev):
    n_b = vec.shape[-1] // B_TILE
    c_tile = 2 * C_TILE
    in_specs = [left_spec(c_tile), pl.BlockSpec((ROW, S_DIM, A_LOC, B_TILE), lambda b, c: (0, 0, 0, b)), MPO_SPEC]
    args = [left_rows, vec, mpo_big]
    alias = {}
    if prev is not None:
        in_specs.append(ANY_SPEC)
        args.append(prev)
        alias = {3: 0}
    return pl.pallas_call(
        stage_one_body,
        grid=(n_b, A_LOC // c_tile),
        in_specs=in_specs,
        out_specs=pl.BlockSpec((W_DIM, S_DIM, c_tile, B_TILE), lambda b, c: (0, 0, c, b + base)),
        out_shape=sds(W_DIM, S_DIM, A_LOC, B_LOC),
        scratch_shapes=[pltpu.VMEM((c_tile * W_DIM, S_DIM * B_TILE), F32)],
        input_output_aliases=alias,
        compiler_params=pltpu.CompilerParams(vmem_limit_bytes=VMEM_LIMIT),
        cost_estimate=stage_one_cost(vec.shape[-1]),
        name='stage_one',
    )(*args)


def stage_one_update_body(step, n_prev, keep, left_ref, mpo_ref, a_hist, b_hist, h_all, *rest):
    gath = rest[:2]
    prev = rest[2:2 + 2 * n_prev]
    rest = rest[2 + 2 * n_prev:]
    out_ref = rest[0]
    kept = rest[1:1 + 2 * keep]
    part_ref, vec, gbuf, pbuf, in_sem, out_sem = rest[1 + 2 * keep:]
    b, c = pl.program_id(0), pl.program_id(1)
    rows = 32

    def loads(tile, s):
        found = [pltpu.make_async_copy(h_all.at[:, s, :, pl.ds(tile * B_TILE, B_TILE)], vec.at[tile, :, s], in_sem.at[tile, s, 0]),
                 pltpu.make_async_copy(gath[tile].at[:, s], gbuf.at[:, s], in_sem.at[tile, s, 1])]
        if n_prev:
            found.append(pltpu.make_async_copy(prev[tile].at[:, s], pbuf.at[:, s], in_sem.at[tile, s, 2]))
        return found

    def saves(tile, s):
        return [pltpu.make_async_copy(vec.at[tile, :, s], kept[tile].at[:, s], out_sem.at[tile, s])] if keep else []

    def update(tile, s):
        for load in loads(tile, s):
            load.wait()
        spread = lambda x: jnp.broadcast_to(x, (rows, B_TILE))
        alpha = spread(a_hist[step:step + 1, 0:1])
        inv = spread(1.0 / b_hist[step:step + 1, 0:1])
        beta_p = spread(b_hist[step - 1:step, 0:1]) if n_prev else None
        for i in range(ROW):
            def body(k, carry):
                r = pl.ds(pl.multiple_of(k * rows, rows), rows)
                w = vec[tile, i, s, r, :] - alpha * gbuf[i, s, r, :]
                if n_prev:
                    w = w - beta_p * pbuf[i, s, r, :]
                vec[tile, i, s, r, :] = w * inv
                return carry

            lax.fori_loop(0, A_LOC // rows, body, 0)

    @pl.when((b == 0) & (c == 0))
    def _():
        for s in range(S_DIM):
            for load in loads(0, s):
                load.start()
        for s in range(S_DIM):
            update(0, s)
        for s in range(S_DIM):
            for load in loads(1, s):
                load.start()

    for s in range(S_DIM):
        @pl.when((b == 0) & (c == 3 + s))
        def _():
            update(1, s)

    if keep:
        for tile in range(2):
            @pl.when((b == tile) & (c == 1))
            def _():
                for s in range(S_DIM):
                    for save in saves(tile, s):
                        save.start()

    first_two_stages(left_ref, lambda i, s: vec[b, i, s], mpo_ref, out_ref, part_ref)

    if keep:
        @pl.when((b == 1) & (c == A_LOC // C_TILE - 1))
        def _():
            for tile in range(2):
                for s in range(S_DIM):
                    for save in saves(tile, s):
                        save.wait()


def stage_one_update(step, left_rows, mpo_big, a_hist, b_hist, h_all, gath, prev, keep):
    n_prev = 0 if prev is None else 1
    args = [left_rows, mpo_big, a_hist, b_hist, h_all] + list(gath) + (list(prev) if n_prev else [])
    tile = (ROW, S_DIM, A_LOC, B_TILE)
    res = pl.pallas_call(
        lambda *refs: stage_one_update_body(step, n_prev, keep, *refs),
        grid=(2, A_LOC // C_TILE),
        in_specs=[left_spec(C_TILE), MPO_SPEC, TILE_SPEC, TILE_SPEC] + [ANY_SPEC] * (3 + 2 * n_prev),
        out_specs=[pl.BlockSpec((W_DIM, S_DIM, C_TILE, B_TILE), lambda b, c: (0, 0, c, b))] + [ANY_SPEC] * (2 * keep),
        out_shape=[sds(W_DIM, S_DIM, A_LOC, B_LOC)] + [sds(*tile)] * (2 * keep),
        scratch_shapes=[
            pltpu.VMEM((C_TILE * W_DIM, S_DIM * B_TILE), F32),
            pltpu.VMEM((2,) + tile, F32),
            pltpu.VMEM(tile, F32),
            pltpu.VMEM(tile if n_prev else (8, 128), F32),
            pltpu.SemaphoreType.DMA((2, S_DIM, 3)),
            pltpu.SemaphoreType.DMA((2, S_DIM)),
        ],
        compiler_params=pltpu.CompilerParams(vmem_limit_bytes=VMEM_LIMIT),
        cost_estimate=stage_one_cost(HALF),
        name='stage_one_update',
    )(*args)
    return res[0], tuple(res[1:])


S3_M = 1024
S3_R = 2


def stage_three_body(has_init, sel_ref, t2_ref, right_ref, *rest):
    out_ref = rest[-1]
    acc = dot(t2_ref[0], right_ref[0])
    for i in range(1, S3_R):
        acc = acc + dot(t2_ref[i], right_ref[i])
    first = pl.program_id(1) == 0
    start = rest[0][...] if has_init else 0.0
    out_ref[...] = jnp.where(first, start, out_ref[...]) + acc


def stage_three(t2, right_t, block, after, init):
    in_specs = [
        pl.BlockSpec((S3_R, S3_M, B_LOC), lambda m, k, sel: (k, m, 0)),
        pl.BlockSpec((S3_R, B_LOC, HALF), lambda m, k, sel: (k, 0, sel[0])),
    ]
    args = [block, t2, right_t]
    if init is not None:
        in_specs.append(pl.BlockSpec((S3_M, HALF), lambda m, k, sel: (m, 0)))
        args.append(init)
    if after is not None:
        in_specs.append(ANY_SPEC)
        args.append(after)
    return pl.pallas_call(
        lambda *refs: stage_three_body(init is not None, *refs),
        grid_spec=pltpu.PrefetchScalarGridSpec(
            num_scalar_prefetch=1,
            grid=(V_ROWS // S3_M, W_DIM // S3_R),
            in_specs=in_specs,
            out_specs=pl.BlockSpec((S3_M, HALF), lambda m, k, sel: (m, 0)),
        ),
        out_shape=sds(V_ROWS, HALF),
        compiler_params=pltpu.CompilerParams(vmem_limit_bytes=VMEM_LIMIT),
        cost_estimate=pl.CostEstimate(flops=STAGE_THREE_FLOPS, bytes_accessed=90 << 20, transcendentals=0),
        name='stage_three',
    )(*args)


def relayout_body(in_ref, out_ref):
    for r in range(W_DIM):
        out_ref[r] = in_ref[:, r, :]


def relayout(right_blk):
    b_t, e_t = B_LOC, 128
    return pl.pallas_call(
        relayout_body,
        grid=(B_LOC // b_t, B_ALL // e_t),
        in_specs=[pl.BlockSpec((b_t, W_DIM, e_t), lambda b, e: (b, 0, e))],
        out_specs=pl.BlockSpec((W_DIM, b_t, e_t), lambda b, e: (0, b, e)),
        out_shape=sds(W_DIM, B_LOC, B_ALL),
        compiler_params=pltpu.CompilerParams(vmem_limit_bytes=VMEM_LIMIT),
        cost_estimate=pl.CostEstimate(flops=1 << 34, bytes_accessed=128 << 20, transcendentals=0),
        name='relayout',
    )(right_blk)


CHUNKS = 8
CH_ROWS = V_ROWS // CHUNKS
STEP_ROWS = 32


def enter_all():
    barrier = pltpu.get_barrier_semaphore()
    me = lax.axis_index('col') * ROW + lax.axis_index('row')
    for d in range(1, NDEV):
        peer = lax.rem(me + d, NDEV)
        pl.semaphore_signal(barrier, inc=1, device_id=(peer // ROW, lax.rem(peer, ROW)), device_id_type=MESH_ID)
    return me, barrier


def all_mean(me, part, slots, send_sem, recv_sem):
    slots[me] = part
    copies = []
    for d in range(1, NDEV):
        peer = lax.rem(me + d, NDEV)
        copy = pltpu.make_async_remote_copy(
            src_ref=slots.at[me], dst_ref=slots.at[me], send_sem=send_sem.at[d], recv_sem=recv_sem.at[me],
            device_id=(peer // ROW, lax.rem(peer, ROW)), device_id_type=MESH_ID)
        copy.start()
        copies.append(copy)
    for d in range(1, NDEV):
        src = lax.rem(me + d, NDEV)
        pltpu.make_async_remote_copy(
            src_ref=slots.at[src], dst_ref=slots.at[src], send_sem=send_sem.at[d], recv_sem=recv_sem.at[src],
            device_id=(src // ROW, lax.rem(src, ROW)), device_id_type=MESH_ID).wait_recv()
    for copy in copies:
        copy.wait_send()
    total = slots[0]
    for i in range(1, NDEV):
        total = total + slots[i]
    total = jnp.sum(jnp.sum(total, axis=0, keepdims=True), axis=1, keepdims=True)
    return jnp.broadcast_to(total, (8, 128)) * (1.0 / NUM_ELEMS)


def fold(x):
    rows = x[0:8]
    for i in range(1, x.shape[0] // 8):
        rows = rows + x[i * 8:(i + 1) * 8]
    out = rows[:, 0:128]
    for i in range(1, rows.shape[1] // 128):
        out = out + rows[:, i * 128:(i + 1) * 128]
    return out


def row_loop(start, rows, body, init):
    def step(i, carry):
        r0 = pl.multiple_of(start + i * STEP_ROWS, STEP_ROWS)
        return body(pl.ds(r0, STEP_ROWS), carry)

    return lax.fori_loop(0, rows // STEP_ROWS, step, init)


def as_scalar_tile(x):
    return jnp.broadcast_to(x[0:1, 0:1], (STEP_ROWS, HALF))


def start_norm_body(psi_ref, out_a1, out_a2, out_c, out_a, vec, in_sem, out_sem, slots, send_sem, recv_sem):
    me, barrier = enter_all()
    loads = []
    per_s = CHUNKS // S_DIM
    for k in range(CHUNKS):
        s, part = k // per_s, k % per_s
        src = psi_ref.at[pl.ds(part * CH_ROWS, CH_ROWS), s // 2, s % 2, :]
        load = pltpu.make_async_copy(src, vec.at[pl.ds(k * CH_ROWS, CH_ROWS), :], in_sem.at[k])
        load.start()
        loads.append(load)
    acc = jnp.zeros((8, 128), F32)
    for k in range(CHUNKS):
        loads[k].wait()

        def body(rows, carry):
            x = vec[rows, :]
            return carry + fold(x * x)

        acc = row_loop(k * CH_ROWS, CH_ROWS, body, acc)
    pl.semaphore_wait(barrier, NDEV - 1)
    inv = lax.rsqrt(all_mean(me, acc, slots, send_sem, recv_sem))
    scale = as_scalar_tile(inv)
    stores = []
    for k in range(CHUNKS):
        def body(rows, carry):
            vec[rows, 0:HALF] = vec[rows, 0:HALF] * scale
            vec[rows, HALF:B_LOC] = vec[rows, HALF:B_LOC] * scale
            return carry

        row_loop(k * CH_ROWS, CH_ROWS, body, 0)
        rows = pl.ds(k * CH_ROWS, CH_ROWS)
        for h, (out, c0, width) in enumerate(((out_a1, 0, B_TILE), (out_a2, B_TILE, B_TILE), (out_c, HALF, HALF), (out_a, 0, HALF))):
            store = pltpu.make_async_copy(vec.at[rows, pl.ds(c0, width)], out.at[rows, :], out_sem.at[h, k])
            store.start()
            stores.append(store)
    for store in stores:
        store.wait()


def start_norm(psi_blk):
    any_spec = pl.BlockSpec(memory_space=pl.ANY)
    return pl.pallas_call(
        start_norm_body,
        in_specs=[any_spec],
        out_specs=[any_spec] * 4,
        out_shape=[sds(V_ROWS, B_TILE), sds(V_ROWS, B_TILE), sds(V_ROWS, HALF), sds(V_ROWS, HALF)],
        scratch_shapes=[
            pltpu.VMEM((V_ROWS, B_LOC), F32),
            pltpu.SemaphoreType.DMA((CHUNKS,)),
            pltpu.SemaphoreType.DMA((4, CHUNKS)),
            pltpu.VMEM((NDEV, 8, 128), F32),
            pltpu.SemaphoreType.DMA((NDEV,)),
            pltpu.SemaphoreType.DMA((NDEV,)),
        ],
        compiler_params=pltpu.CompilerParams(collective_id=0, has_side_effects=True, vmem_limit_bytes=VMEM_LIMIT),
        cost_estimate=pl.CostEstimate(flops=1 << 32, bytes_accessed=16 << 20, transcendentals=0),
        name='start_norm',
    )(psi_blk)


def lanczos_body(step, last, h_a, h_c, v_a, v_c, *rest):
    n_prev = 1 if step else 0
    prevs, rest = rest[:2 * n_prev], rest[2 * n_prev:]
    old, rest = rest[:2 * n_prev], rest[2 * n_prev:]
    n_out = 1 if last else 2
    outs, rest = rest[:n_out], rest[n_out:]
    a_hist, b_hist, hv, vv, pv, in_sem, out_sem, slots, slots2, send_sem, recv_sem, send_sem2, recv_sem2 = rest
    me, barrier = enter_all()
    lo, hi = pl.ds(0, HALF), pl.ds(HALF, HALF)
    loads = []
    for k in range(CHUNKS):
        rows = pl.ds(k * CH_ROWS, CH_ROWS)
        group = []
        moves = [(h_a, hv.at[rows, lo]), (h_c, hv.at[rows, hi]), (v_a, vv.at[rows, lo]), (v_c, vv.at[rows, hi])]
        for i, (src, dst) in enumerate(moves):
            load = pltpu.make_async_copy(src.at[rows, :], dst, in_sem.at[k, i])
            load.start()
            group.append(load)
        loads.append(group)
    late = []
    if n_prev:
        for k in range(CHUNKS):
            rows = pl.ds(k * CH_ROWS, CH_ROWS)
            for i, (src, cols) in enumerate(((prevs[0], lo), (prevs[1], hi))):
                late.append(pltpu.make_async_copy(src.at[rows, :], pv.at[rows, cols], in_sem.at[k, 4 + i]))
    acc = jnp.zeros((8, 128), F32)
    for k in range(CHUNKS):
        for load in loads[k]:
            load.wait()
        if k == CHUNKS // 2:
            for load in late:
                load.start()

        def body(rows, carry):
            return carry + fold(hv[rows, 0:HALF] * vv[rows, 0:HALF] + hv[rows, HALF:B_LOC] * vv[rows, HALF:B_LOC])

        acc = row_loop(k * CH_ROWS, CH_ROWS, body, acc)
    pl.semaphore_wait(barrier, NDEV - 1)
    alpha = all_mean(me, acc, slots, send_sem, recv_sem)
    is_row = lax.broadcasted_iota(jnp.int32, (8, 128), 0) == step
    a_hist[...] = jnp.where(is_row, alpha, old[0][...] if n_prev else 0.0)
    for load in late:
        load.wait()
    alpha_t = as_scalar_tile(alpha)
    beta_t = as_scalar_tile(old[1][step - 1:step, :]) if n_prev else None

    def residual(rows, carry):
        for c0 in (0, HALF):
            w = hv[rows, c0:c0 + HALF] - alpha_t * vv[rows, c0:c0 + HALF]
            if n_prev:
                w = w - beta_t * pv[rows, c0:c0 + HALF]
            hv[rows, c0:c0 + HALF] = w
            carry = carry + fold(w * w)
        return carry

    acc = row_loop(0, V_ROWS, residual, jnp.zeros((8, 128), F32))
    beta = jnp.sqrt(all_mean(me, acc, slots2, send_sem2, recv_sem2))
    b_hist[...] = jnp.where(is_row, beta, old[1][...] if n_prev else 0.0)
    inv_t = as_scalar_tile(1.0 / beta)
    stores = []
    for k in range(CHUNKS):
        def scale_rows(rows, carry):
            for c0 in (0, HALF):
                hv[rows, c0:c0 + HALF] = hv[rows, c0:c0 + HALF] * inv_t
            return carry

        row_loop(k * CH_ROWS, CH_ROWS, scale_rows, 0)
        rows = pl.ds(k * CH_ROWS, CH_ROWS)
        width = B_LOC // n_out
        for h, out in enumerate(outs):
            store = pltpu.make_async_copy(hv.at[rows, pl.ds(h * width, width)], out.at[rows, :], out_sem.at[h, k])
            store.start()
            stores.append(store)
    for store in stores:
        store.wait()


def lanczos_update(step, last, h_a, h_c, v_a, v_c, prev, hist):
    args = [h_a, h_c, v_a, v_c]
    in_specs = [ANY_SPEC] * 4
    if step:
        args += list(prev) + list(hist)
        in_specs += [ANY_SPEC, ANY_SPEC, TILE_SPEC, TILE_SPEC]
    n_out = 1 if last else 2
    big = pltpu.VMEM((V_ROWS, B_LOC), F32)
    return pl.pallas_call(
        lambda *refs: lanczos_body(step, last, *refs),
        in_specs=in_specs,
        out_specs=[ANY_SPEC] * n_out + [TILE_SPEC, TILE_SPEC],
        out_shape=[sds(V_ROWS, B_LOC // n_out)] * n_out + [sds(8, 128), sds(8, 128)],
        scratch_shapes=[
            big, big, big if step else pltpu.VMEM((8, 128), F32),
            pltpu.SemaphoreType.DMA((CHUNKS, 6)),
            pltpu.SemaphoreType.DMA((2, CHUNKS)),
            pltpu.VMEM((NDEV, 8, 128), F32),
            pltpu.VMEM((NDEV, 8, 128), F32),
            pltpu.SemaphoreType.DMA((NDEV,)),
            pltpu.SemaphoreType.DMA((NDEV,)),
            pltpu.SemaphoreType.DMA((NDEV,)),
            pltpu.SemaphoreType.DMA((NDEV,)),
        ],
        compiler_params=pltpu.CompilerParams(collective_id=1 + step, has_side_effects=True, vmem_limit_bytes=VMEM_LIMIT),
        cost_estimate=pl.CostEstimate(flops=1 << 33, bytes_accessed=40 << 20, transcendentals=0),
        name='lanczos_update',
    )(*args)


def gather_rows(x):
    return lax.all_gather(x.reshape(S_DIM, A_LOC, x.shape[-1]), 'row', axis=0, tiled=False)


def solution(mesh):
    swap = [(0, 1), (1, 0)]

    def local_run(psi_blk, left_blk, right_blk, mpo_pair):
        col = lax.axis_index('col').astype(jnp.int32)
        left_rows = left_blk.reshape(A_LOC * W_DIM, A_ALL)
        mpo4 = mpo_pair.reshape(W_DIM, W_DIM, S_DIM, S_DIM).transpose(1, 3, 2, 0)
        same_c = jnp.eye(GROUP, dtype=jnp.bool_)[None, None, :, None, :, None]
        mpo_big = jnp.where(same_c, mpo4[:, :, None, :, None, :], 0.0).reshape(256, 256)

        v_a1, v_a2, v_c, v_a = start_norm(psi_blk)
        gath = (gather_rows(v_a1), gather_rows(v_a2))
        g_c = gather_rows(v_c)
        right_t = relayout(right_blk)
        mine = [(2 * col + i).reshape(1) for i in range(2)]
        theirs = [(2 * (1 - col) + i).reshape(1) for i in range(2)]

        prev = gath_prev = hist = h_all = None
        for step in range(LANCZOS_STEPS):
            last = step == LANCZOS_STEPS - 1
            if step == 0:
                t2 = stage_one(left_rows, gath[0], mpo_big, 0, None)
                t2 = stage_one(left_rows, gath[1], mpo_big, 1, t2)
            else:
                t2, kept = stage_one_update(step - 1, left_rows, mpo_big, *hist, h_all, gath, gath_prev, 0 if last else 1)
                gath, gath_prev = kept, gath
            t2 = stage_one(left_rows, g_c, mpo_big, 2, t2)
            t2 = t2.reshape(W_DIM, V_ROWS, B_LOC)
            oth_a = stage_three(t2, right_t, theirs[0], None, None)
            recv_a = lax.ppermute(oth_a, 'col', swap)
            oth_c = stage_three(t2, right_t, theirs[1], oth_a, None)
            recv_c = lax.ppermute(oth_c, 'col', swap)
            h_a = stage_three(t2, right_t, mine[0], oth_c, recv_a)
            if not last:
                h_all = gather_rows(h_a)
            h_c = stage_three(t2, right_t, mine[1], h_a, recv_c)
            res = lanczos_update(step, last, h_a, h_c, v_a, v_c, prev, hist)
            hist = tuple(res[-2:])
            if not last:
                prev = (v_a, v_c)
                v_a, v_c = res[:2]
                g_c = gather_rows(v_c)
        out = res[0].reshape(S_DIM, A_LOC, B_LOC).transpose(1, 0, 2).reshape(A_LOC, 2, 2, B_LOC)
        return hist[0][:LANCZOS_STEPS, 0], hist[1][:LANCZOS_STEPS, 0], out

    return jax.shard_map(local_run, mesh=mesh, in_specs=(P('row', None, None, 'col'), P('row', None, None), P('col', None, None), P()), out_specs=(P(), P(), P('row', None, None, 'col')), check_vma=False)
```
